32 devices in a mesh: pipe: 4 (over y, x), dp: 8 (over z, core).
Axes of the slice: x: 2, y: 2, z: 4, core: 2. Of those that a mesh axis runs over, the one named last changes fastest.
Arguments:
- acts: bfloat16 [4, 2048, 3072], P('pipe', 'dp'), may hold values from -24 to 24, as said below
- grad: float32 [12288, 4096], P('pipe', 'dp'), may hold values from -6 to 6
- owner_of: int32 [4, 12], replicated, may hold values from 0 to 3, as said below
Outputs:
- precond: float32 [12288, 4096], P('pipe', 'dp')
- held_inverse: float32 [4, 24, 256, 256], P('pipe', None, 'dp')
The draws below stay inside these ranges and needn't reach their ends.
Inputs may be any that keep to these rules, and one draw needn't show every extreme that they name: `acts`: column and token scales of the activations vary; entries lie within the range. `owner_of`: no section index owns more than 24 blocks in all, and some section index owns exactly 24.
All inputs are finite; a program needn't handle non-finite values.
Results may differ from the reference program's by a relative error of at most 0.0003.
Values sent between devices are 32-bit elements; how exact they have to be, the bound alone decides.
A program may use at most 128 MiB of HBM per device.

```python
import math
import jax
import jax.numpy as jnp
from jax import lax

W = 3072
GO = 4096
BLK = 256
NB = 12
HOST = 24
TOKENS = 2048
N_PIPE = 4


def draw_acts(key, part):
    keys = jax.random.split(key, 3)
    shape = (N_PIPE, TOKENS, W)
    col_scale = jnp.exp(jax.random.uniform(keys[1], (N_PIPE, 1, W), jnp.float32, math.log(0.3), math.log(3.0)))
    row_scale = jnp.exp(jax.random.uniform(keys[2], (N_PIPE, TOKENS, 1), jnp.float32, math.log(0.5), math.log(2.0)))
    base = jax.random.normal(keys[0], shape, jnp.float32)
    base = jnp.clip(base, -4.0, 4.0)
    return (base * col_scale * row_scale).astype(jnp.bfloat16)


def draw_owner_of(key, part):
    keys = jax.random.split(jax.random.fold_in(key, 17), 3)
    slot_total = N_PIPE * HOST
    busiest = jax.random.randint(keys[0], (), 0, N_PIPE)
    scores = jax.random.permutation(keys[1], slot_total).astype(jnp.int32)
    slot_ids = jnp.arange(slot_total, dtype=jnp.int32)
    scores = jnp.where(slot_ids // HOST == busiest, scores - slot_total, scores)
    ordered = jnp.argsort(scores, stable=True).astype(jnp.int32)
    chosen = ordered[:N_PIPE * NB] // HOST
    mixing = jax.random.permutation(keys[2], N_PIPE * NB)
    return chosen[mixing].reshape(N_PIPE, NB).astype(jnp.int32)


def block_scale(rng, extent, shards, least, high):
    def one(axis_at, blocks):
        draws = jax.random.uniform(jax.random.fold_in(jax.random.fold_in(rng, 6), axis_at), (blocks,), jnp.float32, least / len(shards), high / len(shards))
        return jnp.repeat(jnp.exp(draws), extent[axis_at] // blocks).reshape((-1,) + (1,) * (len(extent) - axis_at - 1))

    level = one(*shards[0])
    for cut in shards[1:]:
        level = level * one(*cut)
    return level


def noise(stream_key, dims, scale, limit, cuts=(), held_as=jnp.bfloat16):
    result = scale * jax.random.normal(stream_key, dims, jnp.float32)
    if cuts:
        result = result * block_scale(stream_key, dims, cuts, -0.22, 0.18)
    return jnp.clip(result, -limit, limit).astype(held_as)


def setup_inputs(seed: int = 0) -> dict:
    arg_keys = jax.random.split(jax.random.key(seed), 4)
    return {
        "acts": draw_acts(jax.random.fold_in(arg_keys[3], 71), 0),
        "grad": noise(arg_keys[1], (N_PIPE * W, GO), 1.0, 6.0, ((0, 4), (1, 8)), jnp.float32),
        "owner_of": draw_owner_of(jax.random.fold_in(arg_keys[3], 71), 0),
    }


damping_ratio = 0.1

def invert_blocks(factor, vacant):
    order_size = factor.shape[-1]
    diagonal_sum = jnp.sum(jnp.diagonal(factor, axis1=1, axis2=2), axis=1)
    damping = damping_ratio * diagonal_sum / order_size
    identity = jnp.eye(order_size, dtype=factor.dtype)
    shifted = factor + (damping + vacant)[:, None, None] * identity
    cholesky_lower = jnp.linalg.cholesky(shifted)
    identity_stack = jnp.broadcast_to(identity, factor.shape)
    inv_lower = lax.linalg.triangular_solve(cholesky_lower, identity_stack, left_side=True, lower=True)
    return jnp.einsum('mkr,mkc->mrc', inv_lower, inv_lower, precision=lax.Precision.HIGHEST)

def slot_tables(owner_of):
    owners_flat = owner_of.reshape(-1).astype(jnp.int32)
    positions = jnp.arange(owners_flat.shape[0], dtype=jnp.int32)
    matches = owners_flat[:, None] == owners_flat[None, :]
    before = positions[None, :] < positions[:, None]
    slot_rank = jnp.sum((matches & before).astype(jnp.int32), axis=1)
    return (owners_flat, slot_rank)

def reference(acts, grad, owner_of):

    def per_section(section_acts):
        blocks = []
        for block_id in range(NB):
            columns = section_acts[:, block_id * BLK:(block_id + 1) * BLK]
            blocks.append(jnp.dot(columns.T.astype(jnp.float32), columns.astype(jnp.float32), preferred_element_type=jnp.float32))
        factor = jnp.stack(blocks) / TOKENS
        return invert_blocks(factor, jnp.zeros((NB,), factor.dtype))
    inverse = lax.map(per_section, acts)
    precond = jnp.einsum('sbrk,sbkc->sbrc', inverse, grad.reshape(N_PIPE, NB, BLK, GO), precision=lax.Precision.HIGHEST)
    precond = precond.reshape(N_PIPE * W, GO)
    owners_flat, slot_rank = slot_tables(owner_of)
    pipe_ids = jnp.arange(N_PIPE, dtype=jnp.int32)
    slot_ids = jnp.arange(HOST, dtype=jnp.int32)
    selector = (owners_flat[None, None, :] == pipe_ids[:, None, None]) & (slot_rank[None, None, :] == slot_ids[None, :, None])
    selector = selector.astype(inverse.dtype)
    held_inverse = jnp.einsum('pjk,krc->pjrc', selector, inverse.reshape(N_PIPE * NB, BLK, BLK), precision=lax.Precision.HIGHEST)
    return (precond, held_inverse)
```

```python
import functools

import jax
import jax.numpy as jnp
from jax import lax
from jax.experimental import pallas as pl
from jax.experimental.pallas import tpu as pltpu
from jax.sharding import PartitionSpec as P

BLK = 256
HALF = BLK // 2
PACK = 2 * HALF + 8
CHUNKS = 3
CHUNK = PACK // CHUNKS
HOST = 24
UNROLL = 1
MESH = pl.DeviceIdType.MESH

damping_ratio = 0.1
F32 = jnp.float32
BF16 = jnp.bfloat16
HIGHEST = lax.Precision.HIGHEST


def square_iota():
    rows = lax.broadcasted_iota(jnp.int32, (HALF, HALF), 0)
    cols = lax.broadcasted_iota(jnp.int32, (HALF, HALF), 1)
    return rows, cols


def pack_into(ref, m11, m21, m22):
    rows, cols = square_iota()
    diag = jnp.sum(jnp.where(rows == cols, m22, 0.0), axis=0, keepdims=True)
    ref[0:HALF, :] = m21
    ref[HALF:BLK, :] = jnp.where(rows >= cols, m11, m22)
    ref[BLK:PACK, :] = jnp.broadcast_to(diag, (PACK - BLK, HALF))


def unpack(value):
    rows, cols = square_iota()
    m21 = value[0:HALF, :]
    mixed = value[HALF:BLK, :]
    diag = value[BLK : BLK + 1, :]
    turned = mixed.T
    m11 = jnp.where(rows >= cols, mixed, turned)
    m22 = jnp.where(rows < cols, mixed, jnp.where(rows == cols, diag, turned))
    return m11, m21, m22


def greet(signals):
    barrier = pltpu.get_barrier_semaphore()
    for condition, device in signals:
        if condition is None:
            pl.semaphore_signal(barrier, inc=1, device_id=device, device_id_type=MESH)
        else:
            @pl.when(condition)
            def _():
                pl.semaphore_signal(barrier, inc=1, device_id=device, device_id_type=MESH)
    peers = sum(1 if condition is None else condition.astype(jnp.int32) for condition, _ in signals)
    pl.semaphore_wait(barrier, peers)


def dot3(a, b, contract):
    return jnp.stack([
        lax.dot_general(a[i], b[i], (contract, ((), ())), precision=HIGHEST, preferred_element_type=F32)
        for i in range(a.shape[0])
    ])


def sweep_inverse(a):
    count = a.shape[0]
    panel_shape = (count, 8, HALF)
    sub = lax.broadcasted_iota(jnp.int32, panel_shape, 1)
    lane = lax.broadcasted_iota(jnp.int32, panel_shape, 2)
    all_lanes = lax.broadcasted_iota(jnp.int32, (count, HALF, HALF), 2)

    def columns_of(top, first):
        return tuple(jnp.broadcast_to(top[:, :, k : k + 1], panel_shape) for k in range(first, first + 8))

    def panel(_, state):
        a, cols = state
        cols = list(cols)
        top = a[:, 0:8, :]
        for k in range(8):
            here = cols[k]
            inv = jnp.broadcast_to(1.0 / here[:, k : k + 1, :], panel_shape)
            row = jnp.broadcast_to(top[:, k : k + 1, :], panel_shape) * inv
            at_row = sub == k
            new = jnp.where(at_row, row, top - here * row)
            edge = jnp.where(at_row, inv, -here * inv)
            top = jnp.where(lane == k, edge, new)
            for j in range(k + 1, 8):
                across = jnp.broadcast_to(cols[j][:, k : k + 1, :], panel_shape) * inv
                cols[j] = jnp.where(at_row, across, cols[j] - here * across)
        top = jnp.where(lane < 8, -top, top)
        rest = a - jnp.stack([
            lax.dot_general(a[i, 0:8, :], top[i], (((0,), (0,)), ((), ())), precision=HIGHEST, preferred_element_type=F32)
            for i in range(count)
        ])
        ahead = columns_of(rest[:, 8:16, :], 8)
        tall = jnp.concatenate([top, jnp.zeros((count, HALF - 8, HALF), F32)], axis=1)
        turned = jnp.stack([tall[i].T for i in range(count)])
        rest = jnp.where(all_lanes < 8, turned, rest)
        a = jnp.concatenate([rest[:, 8:, :], top], axis=1)
        return pltpu.roll(a, HALF - 8, 2), ahead

    return -lax.fori_loop(0, HALF // 8, panel, (a, columns_of(a[:, 0:8, :], 0)), unroll=UNROLL)[0]


def invert_parts(values, tokens):
    rows, cols = square_iota()
    parts = [unpack(value / tokens) for value in values]
    m11 = jnp.stack([p[0] for p in parts])
    m21 = jnp.stack([p[1] for p in parts])
    m22 = jnp.stack([p[2] for p in parts])
    eye = rows == cols
    trace = jnp.sum(jnp.where(eye, m11 + m22, 0.0), axis=(1, 2), keepdims=True)
    damping = jnp.where(eye, damping_ratio * trace / BLK, 0.0)
    x11 = sweep_inverse(m11 + damping)
    g = dot3(m21, x11, ((1,), (0,)))
    schur = m22 + damping - dot3(g, m21, ((1,), (1,)))
    y = sweep_inverse(schur)
    b21 = -dot3(y, g, ((1,), (0,)))
    b11 = x11 - dot3(g, b21, ((0,), (0,)))
    return b11, b21, y


def solve_kernel(n, sections, nblocks, tokens, acts, grad, precond, rows_out, acts_v, grad_v, theirs, mine, from_pair,
                 inbound, landed, full, acts_s, grad_s, pair_s, pair_r, sum_s, sum_r, line_s, swap_s, near_r,
                 side_s, side_r):
    chips = n // 2
    nhalf = nblocks // 2
    nown = -(-nhalf // 2)
    share = BLK // n
    me = lax.axis_index("dp")
    section = lax.axis_index("pipe")
    core = lax.rem(me, 2)
    chip = me // 2
    pair = me + 1 - 2 * core
    low = (jnp.maximum(chip - 1, 0)) * 2 + core
    high = (jnp.minimum(chip + 1, chips - 1)) * 2 + core
    first = chip == 0
    last = chip == chips - 1
    is_last = last.astype(jnp.int32)

    def acts_copy(t):
        span = pl.ds(pl.multiple_of(t * 2 * BLK, 2 * BLK), 2 * BLK)
        return pltpu.make_async_copy(acts.at[:, span], acts_v.at[:, span], acts_s.at[t])

    def turn_of(p):
        natural = p
        up_first = jnp.where(p < nhalf // 2, 2 * p + 1, 2 * (p - nhalf // 2))
        down_first = jnp.where(p < nown, 2 * p, 2 * (p - nown) + 1)
        return jnp.where(first, up_first, jnp.where(last, down_first, natural))

    for p in range(nhalf):
        acts_copy(turn_of(p)).start()
    grad_copy = pltpu.make_async_copy(grad, grad_v, grad_s)
    grad_copy.start()

    greet(
        [(None, {"dp": pair}), (chip > 0, {"dp": low}), (chip < chips - 1, {"dp": high})]
        + [(None, {"pipe": lax.rem(section + step, sections)}) for step in range(1, sections)]
    )

    def partial(block, ref):
        x = acts_v[:, pl.ds(pl.multiple_of(block * BLK, BLK), BLK)]
        whole = lax.dot_general(x, x, (((0,), (0,)), ((), ())), preferred_element_type=F32)
        pack_into(ref, whole[0:HALF, 0:HALF], whole[HALF:BLK, 0:HALF], whole[HALF:BLK, HALF:BLK])

    def pair_copy(t):
        return pltpu.make_async_remote_copy(
            src_ref=theirs.at[t], dst_ref=from_pair.at[t], send_sem=pair_s.at[t], recv_sem=pair_r.at[t],
            device_id={"dp": pair}, device_id_type=MESH,
        )

    def fold_pair(t):
        pair_copy(t).wait()
        mine[t] = mine[t] + from_pair[t]

    def piece(k):
        return pl.ds(k * CHUNK, CHUNK)

    def sum_copy(t, k, target):
        return pltpu.make_async_remote_copy(
            src_ref=mine.at[t, piece(k)], dst_ref=inbound.at[t, piece(k)], send_sem=sum_s.at[t, k],
            recv_sem=sum_r.at[t, k], device_id={"dp": target}, device_id_type=MESH,
        )

    def pass_sum(t, k, heads, target):
        @pl.when(jnp.logical_not(heads))
        def _():
            sum_copy(t, k, target).wait_recv()
            mine[t, piece(k)] = mine[t, piece(k)] + inbound[t, piece(k)]

        sum_copy(t, k, target).start()

    @pl.loop(0, nown + chips)
    def _(tick):
        for p in (2 * tick, 2 * tick + 1):
            @pl.when(p < nhalf)
            def _():
                t = turn_of(p)
                acts_copy(t).wait()
                partial(2 * t + 1 - core, theirs.at[t])
                pair_copy(t).start()
                partial(2 * t + core, mine.at[t])

        i = tick - 1 - chip
        t = 2 * i + 1
        rising = (i >= 0) & (t < nhalf) & jnp.logical_not(last)
        j = tick - 1 - (chips - 1 - chip)
        u = 2 * j
        falling = (j >= 0) & (u < nhalf) & jnp.logical_not(first)

        @pl.when(rising)
        def _():
            fold_pair(t)

        @pl.when(falling)
        def _():
            fold_pair(u)

        for k in range(CHUNKS):
            @pl.when(rising)
            def _():
                pass_sum(t, k, first, high)

            @pl.when(falling)
            def _():
                pass_sum(u, k, last, low)

    def close_sum(t):
        fold_pair(t)
        for k in range(CHUNKS):
            sum_copy(t, k, low).wait_recv()
        return mine[t] + inbound[t]

    def invert(slots):
        own = [2 * slot + is_last for slot in slots]
        b11, b21, b22 = invert_parts([close_sum(t) for t in own], tokens)
        for i, t in enumerate(own):
            pack_into(landed.at[2 * t + core], b11[i], b21[i], b22[i])

    def send(t, half, k, target, sem):
        block = 2 * t + half
        return pltpu.make_async_remote_copy(
            src_ref=landed.at[block, piece(k)], dst_ref=landed.at[block, piece(k)], send_sem=sem.at[t, k],
            recv_sem=near_r.at[block, k], device_id={"dp": target}, device_id_type=MESH,
        )

    def flow(t, k, owned, ends, target):
        @pl.when(jnp.logical_not(owned))
        def _():
            send(t, core, k, pair, swap_s).wait_recv()

        @pl.when(jnp.logical_not(ends))
        def _():
            send(t, core, k, target, line_s).start()

        send(t, core, k, pair, swap_s).start()

    def side(block, step):
        mine_rows = full.at[block, pl.ds(pl.multiple_of(me * share, share), share), :]
        return pltpu.make_async_remote_copy(
            src_ref=mine_rows, dst_ref=rows_out.at[section, block], send_sem=side_s.at[block, step - 1],
            recv_sem=side_r.at[section, block],
            device_id={"pipe": lax.rem(section + step, sections)}, device_id_type=MESH,
        )

    def open_block(block):
        m11, m21, m22 = unpack(landed[block])
        full[block, 0:HALF, 0:HALF] = m11
        full[block, HALF:BLK, 0:HALF] = m21
        full[block, 0:HALF, HALF:BLK] = m21.T
        full[block, HALF:BLK, HALF:BLK] = m22
        for step in range(1, sections):
            side(block, step).start()
        rows_out[section, block] = full[block, pl.ds(pl.multiple_of(me * share, share), share), :]

    def open_other(t):
        for k in range(CHUNKS):
            send(t, 1 - core, k, pair, swap_s).wait_recv()
        open_block(2 * t + 1 - core)

    def product(block):
        span = pl.ds(pl.multiple_of(block * BLK, BLK), BLK)
        a = full[block]
        b = grad_v[span, :]
        a_high = a.astype(BF16)
        a_low = (a - a_high.astype(F32)).astype(BF16)
        b_high = b.astype(BF16)
        b_low = (b - b_high.astype(F32)).astype(BF16)
        small = jnp.dot(a_high, b_low, preferred_element_type=F32) + jnp.dot(a_low, b_high, preferred_element_type=F32)
        precond[span, :] = jnp.dot(a_high, b_high, preferred_element_type=F32) + small

    def both_products(t):
        @pl.loop(0, 2)
        def _(half):
            product(2 * t + half)

    @pl.loop(0, nown + chips)
    def _(tick):
        i = tick - chip
        t = 2 * i
        rising = (i >= 0) & (t < nhalf)
        j = tick - (chips - 1 - chip)
        u = 2 * j + 1
        falling = (j >= 0) & (u < nhalf)
        rose = (i >= 1) & (t - 2 < nhalf)
        fell = (j >= 1) & (u - 2 < nhalf)

        @pl.when((tick == 0) & (first | last))
        def _():
            invert([0])

        @pl.when((tick == 1) & (first | last))
        def _():
            invert(list(range(1, nown)))

        for k in range(CHUNKS):
            @pl.when(rising)
            def _():
                flow(t, k, first, last, high)

            @pl.when(falling)
            def _():
                flow(u, k, last, first, low)

            if k == 0:
                @pl.when(rose)
                def _():
                    open_other(t - 2)

                @pl.when(fell)
                def _():
                    open_other(u - 2)

                @pl.when(tick == 1)
                def _():
                    grad_copy.wait()

            if k == 1:
                @pl.when(rose)
                def _():
                    both_products(t - 2)

            if k == 2:
                @pl.when(rising)
                def _():
                    open_block(2 * t + core)

                @pl.when(falling)
                def _():
                    open_block(2 * u + core)

                @pl.when(fell)
                def _():
                    both_products(u - 2)

    @pl.loop(0, nhalf)
    def _(t):
        odd = lax.rem(t, 2) == 1
        sends_sum = jnp.where(odd, jnp.logical_not(last), jnp.logical_not(first))
        sends_inverse = jnp.where(odd, jnp.logical_not(first), jnp.logical_not(last))
        for k in range(CHUNKS):
            @pl.when(sends_sum)
            def _():
                sum_copy(t, k, low).wait_send()

            @pl.when(sends_inverse)
            def _():
                send(t, core, k, low, line_s).wait_send()

            send(t, core, k, pair, swap_s).wait_send()

    @pl.loop(0, nblocks)
    def _(block):
        for step in range(1, sections):
            side(block, step).wait_send()
            source = lax.rem(section + step, sections)
            pltpu.make_async_remote_copy(
                src_ref=rows_out.at[source, block], dst_ref=rows_out.at[source, block],
                send_sem=side_s.at[block, step - 1], recv_sem=side_r.at[source, block],
                device_id={"pipe": source}, device_id_type=MESH,
            ).wait_recv()


def emit_kernel(owners, values, rows, precond, held, slots, zeros, copy_s, held_s):
    section = lax.axis_index("pipe")
    sections, nblocks = owners.shape
    total = sections * nblocks
    zeros[...] = jnp.zeros_like(zeros)

    def precond_copy(b):
        span = pl.ds(pl.multiple_of(b * BLK, BLK), BLK)
        return pltpu.make_async_copy(values.at[span, :], precond.at[span, :], copy_s.at[b])

    for b in range(nblocks):
        precond_copy(b).start()

    for j in range(HOST):
        slots[j] = -1

    def place(k, used):
        hit = owners[k // nblocks, lax.rem(k, nblocks)] == section

        @pl.when(hit)
        def _():
            slots[used] = k

        return used + hit.astype(jnp.int32)

    lax.fori_loop(0, total, place, jnp.int32(0))

    @pl.loop(0, HOST)
    def _(j):
        k = slots[j]

        @pl.when(k >= 0)
        def _():
            pltpu.make_async_copy(rows.at[k // nblocks, lax.rem(k, nblocks)], held.at[j], held_s.at[j]).start()

        @pl.when(k < 0)
        def _():
            pltpu.make_async_copy(zeros, held.at[j], held_s.at[j]).start()

    @pl.loop(0, HOST)
    def _(j):
        pltpu.make_async_copy(zeros, held.at[j], held_s.at[j]).wait()

    for b in range(nblocks):
        precond_copy(b).wait()


def shards(acts, grad, owner_of):
    tokens, feature_count = acts.shape[1:]
    columns = grad.shape[1]
    nblocks = feature_count // BLK
    n = lax.axis_size("dp")
    sections = lax.axis_size("pipe")
    nhalf = nblocks // 2
    share = BLK // n
    vmem = pl.BlockSpec(memory_space=pltpu.VMEM)
    hbm = pl.BlockSpec(memory_space=pltpu.HBM)
    smem = pl.BlockSpec(memory_space=pltpu.SMEM)
    dma = pltpu.SemaphoreType.DMA

    values, rows = pl.pallas_call(
        functools.partial(solve_kernel, n, sections, nblocks, float(tokens * n)),
        out_shape=(
            pltpu.VMEM((feature_count, columns), F32),
            pltpu.VMEM((sections, nblocks, share, BLK), F32),
        ),
        in_specs=[hbm, hbm],
        out_specs=(vmem, vmem),
        scratch_shapes=[
            pltpu.VMEM((tokens, feature_count), BF16),
            pltpu.VMEM((feature_count, columns), F32),
            pltpu.VMEM((nhalf, PACK, HALF), F32),
            pltpu.VMEM((nhalf, PACK, HALF), F32),
            pltpu.VMEM((nhalf, PACK, HALF), F32),
            pltpu.VMEM((nhalf, PACK, HALF), F32),
            pltpu.VMEM((nblocks, PACK, HALF), F32),
            pltpu.VMEM((nblocks, BLK, BLK), F32),
            dma((nhalf,)), dma, dma((nhalf,)), dma((nhalf,)), dma((nhalf, CHUNKS)), dma((nhalf, CHUNKS)),
            dma((nhalf, CHUNKS)), dma((nhalf, CHUNKS)), dma((nblocks, CHUNKS)),
            dma((nblocks, sections - 1)), dma((sections, nblocks)),
        ],
        compiler_params=pltpu.CompilerParams(collective_id=0, has_side_effects=True, vmem_limit_bytes=36 * 2**20),
        name="solve_blocks",
    )(pltpu.with_memory_space_constraint(acts[0], pltpu.HBM), pltpu.with_memory_space_constraint(grad, pltpu.HBM))

    precond, held = pl.pallas_call(
        emit_kernel,
        in_specs=[smem, vmem, vmem],
        out_specs=(hbm, hbm),
        out_shape=(
            jax.ShapeDtypeStruct((feature_count, columns), F32),
            jax.ShapeDtypeStruct((HOST, share, BLK), F32),
        ),
        scratch_shapes=[pltpu.SMEM((HOST,), jnp.int32), pltpu.VMEM((share, BLK), F32), dma((nblocks,)), dma((HOST,))],
        compiler_params=pltpu.CompilerParams(vmem_limit_bytes=16 * 2**20),
        name="emit_outputs",
    )(owner_of, values, rows)
    return precond, held[None]


def solution(mesh):
    placed = (P("pipe", "dp", None), P("pipe", "dp"), P())
    return jax.shard_map(
        shards,
        mesh=mesh,
        in_specs=placed,
        out_specs=(P("pipe", "dp"), P("pipe", None, "dp", None)),
        check_vma=False,
    )
```

```python
import functools

import jax
import jax.numpy as jnp
from jax import lax
from jax.experimental import pallas as pl
from jax.experimental.pallas import tpu as pltpu
from jax.sharding import PartitionSpec as P

BLK = 256
HALF = BLK // 2
PACK = 2 * HALF + 8
CHUNKS = 3
CHUNK = PACK // CHUNKS
HOST = 24
PANEL = 16
UNROLL = 1
MESH = pl.DeviceIdType.MESH

damping_ratio = 0.1
F32 = jnp.float32
BF16 = jnp.bfloat16
HIGHEST = lax.Precision.HIGHEST


def square_iota():
    rows = lax.broadcasted_iota(jnp.int32, (HALF, HALF), 0)
    cols = lax.broadcasted_iota(jnp.int32, (HALF, HALF), 1)
    return rows, cols


def pack_into(ref, m11, m21, m22):
    rows, cols = square_iota()
    diag = jnp.sum(jnp.where(rows == cols, m22, 0.0), axis=0, keepdims=True)
    ref[0:HALF, :] = m21
    ref[HALF:BLK, :] = jnp.where(rows >= cols, m11, m22)
    ref[BLK:PACK, :] = jnp.broadcast_to(diag, (PACK - BLK, HALF))


def unpack(value):
    rows, cols = square_iota()
    m21 = value[0:HALF, :]
    mixed = value[HALF:BLK, :]
    diag = value[BLK : BLK + 1, :]
    turned = mixed.T
    m11 = jnp.where(rows >= cols, mixed, turned)
    m22 = jnp.where(rows < cols, mixed, jnp.where(rows == cols, diag, turned))
    return m11, m21, m22


def greet(signals):
    barrier = pltpu.get_barrier_semaphore()
    for condition, device in signals:
        if condition is None:
            pl.semaphore_signal(barrier, inc=1, device_id=device, device_id_type=MESH)
        else:
            @pl.when(condition)
            def _():
                pl.semaphore_signal(barrier, inc=1, device_id=device, device_id_type=MESH)
    peers = sum(1 if condition is None else condition.astype(jnp.int32) for condition, _ in signals)
    pl.semaphore_wait(barrier, peers)


def thirds(x):
    high = x.astype(BF16)
    rest = x - high.astype(F32)
    mid = rest.astype(BF16)
    return high, mid, (rest - mid.astype(F32)).astype(BF16)


def wide_dot(left, right):
    lh, lm, ll = thirds(left)
    rh, rm, rl = thirds(right)
    return lax.dot_general(
        jnp.concatenate([lh, lh, lm, lh, lm, ll], axis=0), jnp.concatenate([rh, rm, rh, rl, rm, rh], axis=0),
        (((0,), (0,)), ((), ())), preferred_element_type=F32,
    )


def sweep_inverse(blocks):
    groups = PANEL // 8
    sub = lax.broadcasted_iota(jnp.int32, (8, HALF), 0)
    lane = lax.broadcasted_iota(jnp.int32, (8, HALF), 1)
    all_lanes = lax.broadcasted_iota(jnp.int32, (HALF, HALF), 1)

    def splat(value, row):
        return jnp.broadcast_to(value[row : row + 1, :], (8, HALF))

    def columns_of(rows, at):
        return tuple(
            tuple(jnp.broadcast_to(rows[8 * g : 8 * g + 8, at + j : at + j + 1], (8, HALF)) for g in range(groups))
            for j in range(PANEL)
        )

    def pivots(a, cols):
        cols = [list(c) for c in cols]
        top = [jnp.where(lane < PANEL, (lane == sub + 8 * g).astype(F32), a[8 * g : 8 * g + 8, :]) for g in range(groups)]
        for k in range(PANEL):
            at, row = k // 8, k % 8
            here = cols[k]
            inv = 1.0 / splat(here[at], row)
            hit = sub == row
            scaled = [jnp.where(hit, -inv, here[g] * inv) if g == at else here[g] * inv for g in range(groups)]

            def eliminate(target):
                lead = splat(target[at], row)
                return [
                    (jnp.where(hit, 0.0, target[g]) if g == at else target[g]) - scaled[g] * lead for g in range(groups)
                ]

            for j in range(k + 1, PANEL):
                cols[j] = eliminate(cols[j])
            top = eliminate(top)
        return jnp.concatenate([jnp.where(lane < PANEL, -t, t) for t in top], axis=0)

    def update(a, top, near):
        ahead = [jnp.where(lane < PANEL, 0.0, a[PANEL + 8 * g : PANEL + 8 * g + 8, :]) for g in range(groups)]
        for g in range(groups):
            terms = [near[k][g] * splat(top[8 * (k // 8) : 8 * (k // 8) + 8, :], k % 8) for k in range(PANEL)]
            while len(terms) > 1:
                terms = [terms[i] + terms[i + 1] for i in range(0, len(terms), 2)]
            ahead[g] = ahead[g] - terms[0]
        ahead = jnp.concatenate(ahead, axis=0)
        below = jnp.where(all_lanes[2 * PANEL :, :] < PANEL, 0.0, a[2 * PANEL :, :]) - wide_dot(a[0:PANEL, 2 * PANEL :], top)
        cols = columns_of(ahead, PANEL)
        return pltpu.roll(jnp.concatenate([ahead, below, top], axis=0), HALF - PANEL, 1), cols

    def panel(_, state):
        out = []
        for a, cols in state:
            near = columns_of(a[PANEL : 2 * PANEL, :], 0)
            top = pivots(a, cols)
            out.append(update(a, top, near))
        return tuple(out)

    start = tuple((a, columns_of(a[0:PANEL, :], 0)) for a in blocks)
    return [-a for a, _ in lax.fori_loop(0, HALF // PANEL, panel, start, unroll=UNROLL)]


def high_dot(a, b, contract):
    return lax.dot_general(a, b, (contract, ((), ())), precision=HIGHEST, preferred_element_type=F32)


def invert_dense(m11, m21, m22):
    count=len(m11)
    x11 = sweep_inverse(m11)
    g = [high_dot(m21[i], x11[i], ((1,), (0,))) for i in range(count)]
    y = sweep_inverse([m22[i] - high_dot(g[i], m21[i], ((1,), (1,))) for i in range(count)])
    b21 = [-high_dot(y[i], g[i], ((1,), (0,))) for i in range(count)]
    b11 = [x11[i] - high_dot(g[i], b21[i], ((0,), (0,))) for i in range(count)]
    return b11, b21, y


def invert_parts(values, tokens):
    rows, cols = square_iota()
    eye = rows == cols
    m11, m21, m22 = [], [], []
    for value in values:
        p11, p21, p22 = unpack(value / tokens)
        damping = damping_ratio * jnp.sum(jnp.where(eye, p11 + p22, 0.0), axis=(0, 1), keepdims=True) / BLK
        m11.append(p11 + jnp.where(eye, damping, 0.0))
        m21.append(p21)
        m22.append(p22 + jnp.where(eye, damping, 0.0))
    return invert_dense(m11, m21, m22)


def solve_kernel(n, sections, nblocks, tokens, acts, grad, precond, rows_out, acts_v, grad_v, theirs, mine, from_pair,
                 inbound, landed, full, acts_s, grad_s, pair_s, pair_r, sum_s, sum_r, line_s, swap_s, near_r,
                 side_s, side_r):
    chips = n // 2
    nhalf = nblocks // 2
    nown = -(-nhalf // 2)
    share = BLK // n
    me = lax.axis_index("dp")
    section = lax.axis_index("pipe")
    core = lax.rem(me, 2)
    chip = me // 2
    pair = me + 1 - 2 * core
    low = (jnp.maximum(chip - 1, 0)) * 2 + core
    high = (jnp.minimum(chip + 1, chips - 1)) * 2 + core
    first = chip == 0
    last = chip == chips - 1
    is_last = last.astype(jnp.int32)

    def acts_copy(t):
        span = pl.ds(pl.multiple_of(t * 2 * BLK, 2 * BLK), 2 * BLK)
        return pltpu.make_async_copy(acts.at[:, span], acts_v.at[:, span], acts_s.at[t])

    def turn_of(p):
        natural = p
        up_first = jnp.where(p < nhalf // 2, 2 * p + 1, 2 * (p - nhalf // 2))
        down_first = jnp.where(p < nown, 2 * p, 2 * (p - nown) + 1)
        return jnp.where(first, up_first, jnp.where(last, down_first, natural))

    for p in range(nhalf):
        acts_copy(turn_of(p)).start()
    grad_copy = pltpu.make_async_copy(grad, grad_v, grad_s)
    grad_copy.start()

    greet(
        [(None, {"dp": pair}), (chip > 0, {"dp": low}), (chip < chips - 1, {"dp": high})]
        + [(None, {"pipe": lax.rem(section + step, sections)}) for step in range(1, sections)]
    )

    def partial(block, ref):
        x = acts_v[:, pl.ds(pl.multiple_of(block * BLK, BLK), BLK)]
        whole = lax.dot_general(x, x, (((0,), (0,)), ((), ())), preferred_element_type=F32)
        pack_into(ref, whole[0:HALF, 0:HALF], whole[HALF:BLK, 0:HALF], whole[HALF:BLK, HALF:BLK])

    def pair_copy(t):
        return pltpu.make_async_remote_copy(
            src_ref=theirs.at[t], dst_ref=from_pair.at[t], send_sem=pair_s.at[t], recv_sem=pair_r.at[t],
            device_id={"dp": pair}, device_id_type=MESH,
        )

    def fold_pair(t):
        pair_copy(t).wait()
        mine[t] = mine[t] + from_pair[t]

    def piece(k):
        return pl.ds(k * CHUNK, CHUNK)

    def sum_copy(t, k, target):
        return pltpu.make_async_remote_copy(
            src_ref=mine.at[t, piece(k)], dst_ref=inbound.at[t, piece(k)], send_sem=sum_s.at[t, k],
            recv_sem=sum_r.at[t, k], device_id={"dp": target}, device_id_type=MESH,
        )

    def pass_sum(t, k, heads, target):
        @pl.when(jnp.logical_not(heads))
        def _():
            sum_copy(t, k, target).wait_recv()
            mine[t, piece(k)] = mine[t, piece(k)] + inbound[t, piece(k)]

        sum_copy(t, k, target).start()

    @pl.loop(0, nown + chips)
    def _(tick):
        for p in (2 * tick, 2 * tick + 1):
            @pl.when(p < nhalf)
            def _():
                t = turn_of(p)
                acts_copy(t).wait()
                partial(2 * t + 1 - core, theirs.at[t])
                pair_copy(t).start()
                partial(2 * t + core, mine.at[t])

        i = tick - 1 - chip
        t = 2 * i + 1
        rising = (i >= 0) & (t < nhalf) & jnp.logical_not(last)
        j = tick - 1 - (chips - 1 - chip)
        u = 2 * j
        falling = (j >= 0) & (u < nhalf) & jnp.logical_not(first)

        @pl.when(rising)
        def _():
            fold_pair(t)

        @pl.when(falling)
        def _():
            fold_pair(u)

        for k in range(CHUNKS):
            @pl.when(rising)
            def _():
                pass_sum(t, k, first, high)

            @pl.when(falling)
            def _():
                pass_sum(u, k, last, low)

    def close_sum(t):
        fold_pair(t)
        for k in range(CHUNKS):
            sum_copy(t, k, low).wait_recv()
        return mine[t] + inbound[t]

    def invert(slots):
        own = [2 * slot + is_last for slot in slots]
        b11, b21, b22 = invert_parts([close_sum(t) for t in own], tokens)
        for i, t in enumerate(own):
            pack_into(landed.at[2 * t + core], b11[i], b21[i], b22[i])

    def send(t, half, k, target, sem):
        block = 2 * t + half
        return pltpu.make_async_remote_copy(
            src_ref=landed.at[block, piece(k)], dst_ref=landed.at[block, piece(k)], send_sem=sem.at[t, k],
            recv_sem=near_r.at[block, k], device_id={"dp": target}, device_id_type=MESH,
        )

    def flow(t, k, owned, ends, target):
        @pl.when(jnp.logical_not(owned))
        def _():
            send(t, core, k, pair, swap_s).wait_recv()

        @pl.when(jnp.logical_not(ends))
        def _():
            send(t, core, k, target, line_s).start()

        send(t, core, k, pair, swap_s).start()

    def side(block, step):
        mine_rows = full.at[block, pl.ds(pl.multiple_of(me * share, share), share), :]
        return pltpu.make_async_remote_copy(
            src_ref=mine_rows, dst_ref=rows_out.at[section, block], send_sem=side_s.at[block, step - 1],
            recv_sem=side_r.at[section, block],
            device_id={"pipe": lax.rem(section + step, sections)}, device_id_type=MESH,
        )

    def open_block(block):
        m11, m21, m22 = unpack(landed[block])
        full[block, 0:HALF, 0:HALF] = m11
        full[block, HALF:BLK, 0:HALF] = m21
        full[block, 0:HALF, HALF:BLK] = m21.T
        full[block, HALF:BLK, HALF:BLK] = m22
        for step in range(1, sections):
            side(block, step).start()
        rows_out[section, block] = full[block, pl.ds(pl.multiple_of(me * share, share), share), :]

    def open_other(t):
        for k in range(CHUNKS):
            send(t, 1 - core, k, pair, swap_s).wait_recv()
        open_block(2 * t + 1 - core)

    def product(block):
        span = pl.ds(pl.multiple_of(block * BLK, BLK), BLK)
        a = full[block]
        b = grad_v[span, :]
        a_high = a.astype(BF16)
        a_low = (a - a_high.astype(F32)).astype(BF16)
        b_high = b.astype(BF16)
        b_low = (b - b_high.astype(F32)).astype(BF16)
        small = jnp.dot(a_high, b_low, preferred_element_type=F32) + jnp.dot(a_low, b_high, preferred_element_type=F32)
        precond[span, :] = jnp.dot(a_high, b_high, preferred_element_type=F32) + small

    def both_products(t):
        @pl.loop(0, 2)
        def _(half):
            product(2 * t + half)

    @pl.loop(0, nown + chips)
    def _(tick):
        i = tick - chip
        t = 2 * i
        rising = (i >= 0) & (t < nhalf)
        j = tick - (chips - 1 - chip)
        u = 2 * j + 1
        falling = (j >= 0) & (u < nhalf)
        rose = (i >= 1) & (t - 2 < nhalf)
        fell = (j >= 1) & (u - 2 < nhalf)

        @pl.when((tick == 0) & (first | last))
        def _():
            invert([0])

        @pl.when((tick == 1) & (first | last))
        def _():
            invert(list(range(1, nown)))

        for k in range(CHUNKS):
            @pl.when(rising)
            def _():
                flow(t, k, first, last, high)

            @pl.when(falling)
            def _():
                flow(u, k, last, first, low)

            if k == 0:
                @pl.when(rose)
                def _():
                    open_other(t - 2)

                @pl.when(fell)
                def _():
                    open_other(u - 2)

                @pl.when(tick == 1)
                def _():
                    grad_copy.wait()

            if k == 1:
                @pl.when(rose)
                def _():
                    both_products(t - 2)

            if k == 2:
                @pl.when(rising)
                def _():
                    open_block(2 * t + core)

                @pl.when(falling)
                def _():
                    open_block(2 * u + core)

                @pl.when(fell)
                def _():
                    both_products(u - 2)

    @pl.loop(0, nhalf)
    def _(t):
        odd = lax.rem(t, 2) == 1
        sends_sum = jnp.where(odd, jnp.logical_not(last), jnp.logical_not(first))
        sends_inverse = jnp.where(odd, jnp.logical_not(first), jnp.logical_not(last))
        for k in range(CHUNKS):
            @pl.when(sends_sum)
            def _():
                sum_copy(t, k, low).wait_send()

            @pl.when(sends_inverse)
            def _():
                send(t, core, k, low, line_s).wait_send()

            send(t, core, k, pair, swap_s).wait_send()

    @pl.loop(0, nblocks)
    def _(block):
        for step in range(1, sections):
            side(block, step).wait_send()
            source = lax.rem(section + step, sections)
            pltpu.make_async_remote_copy(
                src_ref=rows_out.at[source, block], dst_ref=rows_out.at[source, block],
                send_sem=side_s.at[block, step - 1], recv_sem=side_r.at[source, block],
                device_id={"pipe": source}, device_id_type=MESH,
            ).wait_recv()


def emit_kernel(owners, values, rows, precond, held, slots, zeros, copy_s, held_s):
    section = lax.axis_index("pipe")
    sections, nblocks = owners.shape
    total = sections * nblocks
    zeros[...] = jnp.zeros_like(zeros)

    def precond_copy(b):
        span = pl.ds(pl.multiple_of(b * BLK, BLK), BLK)
        return pltpu.make_async_copy(values.at[span, :], precond.at[span, :], copy_s.at[b])

    for b in range(nblocks):
        precond_copy(b).start()

    for j in range(HOST):
        slots[j] = -1

    def place(k, used):
        hit = owners[k // nblocks, lax.rem(k, nblocks)] == section

        @pl.when(hit)
        def _():
            slots[used] = k

        return used + hit.astype(jnp.int32)

    lax.fori_loop(0, total, place, jnp.int32(0))

    @pl.loop(0, HOST)
    def _(j):
        k = slots[j]

        @pl.when(k >= 0)
        def _():
            pltpu.make_async_copy(rows.at[k // nblocks, lax.rem(k, nblocks)], held.at[j], held_s.at[j]).start()

        @pl.when(k < 0)
        def _():
            pltpu.make_async_copy(zeros, held.at[j], held_s.at[j]).start()

    @pl.loop(0, HOST)
    def _(j):
        pltpu.make_async_copy(zeros, held.at[j], held_s.at[j]).wait()

    for b in range(nblocks):
        precond_copy(b).wait()


def shards(acts, grad, owner_of):
    tokens, feature_count = acts.shape[1:]
    columns = grad.shape[1]
    nblocks = feature_count // BLK
    n = lax.axis_size("dp")
    sections = lax.axis_size("pipe")
    nhalf = nblocks // 2
    share = BLK // n
    vmem = pl.BlockSpec(memory_space=pltpu.VMEM)
    hbm = pl.BlockSpec(memory_space=pltpu.HBM)
    smem = pl.BlockSpec(memory_space=pltpu.SMEM)
    dma = pltpu.SemaphoreType.DMA

    values, rows = pl.pallas_call(
        functools.partial(solve_kernel, n, sections, nblocks, float(tokens * n)),
        out_shape=(
            pltpu.VMEM((feature_count, columns), F32),
            pltpu.VMEM((sections, nblocks, share, BLK), F32),
        ),
        in_specs=[hbm, hbm],
        out_specs=(vmem, vmem),
        scratch_shapes=[
            pltpu.VMEM((tokens, feature_count), BF16),
            pltpu.VMEM((feature_count, columns), F32),
            pltpu.VMEM((nhalf, PACK, HALF), F32),
            pltpu.VMEM((nhalf, PACK, HALF), F32),
            pltpu.VMEM((nhalf, PACK, HALF), F32),
            pltpu.VMEM((nhalf, PACK, HALF), F32),
            pltpu.VMEM((nblocks, PACK, HALF), F32),
            pltpu.VMEM((nblocks, BLK, BLK), F32),
            dma((nhalf,)), dma, dma((nhalf,)), dma((nhalf,)), dma((nhalf, CHUNKS)), dma((nhalf, CHUNKS)),
            dma((nhalf, CHUNKS)), dma((nhalf, CHUNKS)), dma((nblocks, CHUNKS)),
            dma((nblocks, sections - 1)), dma((sections, nblocks)),
        ],
        compiler_params=pltpu.CompilerParams(collective_id=0, has_side_effects=True, vmem_limit_bytes=36 * 2**20),
        name="solve_blocks",
    )(pltpu.with_memory_space_constraint(acts[0], pltpu.HBM), pltpu.with_memory_space_constraint(grad, pltpu.HBM))

    precond, held = pl.pallas_call(
        emit_kernel,
        in_specs=[smem, vmem, vmem],
        out_specs=(hbm, hbm),
        out_shape=(
            jax.ShapeDtypeStruct((feature_count, columns), F32),
            jax.ShapeDtypeStruct((HOST, share, BLK), F32),
        ),
        scratch_shapes=[pltpu.SMEM((HOST,), jnp.int32), pltpu.VMEM((share, BLK), F32), dma((nblocks,)), dma((HOST,))],
        compiler_params=pltpu.CompilerParams(vmem_limit_bytes=16 * 2**20),
        name="emit_outputs",
    )(owner_of, values, rows)
    return precond, held[None]


def solution(mesh):
    placed = (P("pipe", "dp", None), P("pipe", "dp"), P())
    return jax.shard_map(
        shards,
        mesh=mesh,
        in_specs=placed,
        out_specs=(P("pipe", "dp"), P("pipe", None, "dp", None)),
        check_vma=False,
    )
```

```python
import functools

import jax
import jax.numpy as jnp
from jax import lax
from jax.experimental import pallas as pl
from jax.experimental.pallas import tpu as pltpu
from jax.sharding import PartitionSpec as P

BLK = 256
HALF = BLK // 2
PACK = 2 * HALF + 8
PIECES = tuple((88 * i, 88) for i in range(3))
CHUNKS = len(PIECES)
HOST = 24
PANEL = 16
UNROLL = 1
MESH = pl.DeviceIdType.MESH

damping_ratio = 0.1
F32 = jnp.float32
BF16 = jnp.bfloat16
HIGHEST = lax.Precision.HIGHEST


def square_iota():
    rows = lax.broadcasted_iota(jnp.int32, (HALF, HALF), 0)
    cols = lax.broadcasted_iota(jnp.int32, (HALF, HALF), 1)
    return rows, cols


def pack_into(ref, m11, m21, m22):
    rows, cols = square_iota()
    diag = jnp.sum(jnp.where(rows == cols, m22, 0.0), axis=0, keepdims=True)
    ref[0:HALF, :] = m21
    ref[HALF:BLK, :] = jnp.where(rows >= cols, m11, m22)
    ref[BLK:PACK, :] = jnp.broadcast_to(diag, (PACK - BLK, HALF))


def unpack(value):
    rows, cols = square_iota()
    m21 = value[0:HALF, :]
    mixed = value[HALF:BLK, :]
    diag = value[BLK : BLK + 1, :]
    turned = mixed.T
    m11 = jnp.where(rows >= cols, mixed, turned)
    m22 = jnp.where(rows < cols, mixed, jnp.where(rows == cols, diag, turned))
    return m11, m21, m22


def greet(signals):
    barrier = pltpu.get_barrier_semaphore()
    for condition, device in signals:
        if condition is None:
            pl.semaphore_signal(barrier, inc=1, device_id=device, device_id_type=MESH)
        else:
            @pl.when(condition)
            def _():
                pl.semaphore_signal(barrier, inc=1, device_id=device, device_id_type=MESH)
    peers = sum(1 if condition is None else condition.astype(jnp.int32) for condition, _ in signals)
    return lambda: pl.semaphore_wait(barrier, peers)


def thirds(x):
    high = x.astype(BF16)
    rest = x - high.astype(F32)
    mid = rest.astype(BF16)
    return high, mid, (rest - mid.astype(F32)).astype(BF16)


def wide_dot(left, right):
    lefts, rights = [], []
    for l, r in zip(left, right):
        lh, lm, ll = thirds(l)
        rh, rm, rl = thirds(r)
        lefts += [lh, lh, lm, lh, lm, ll]
        rights += [rh, rm, rh, rl, rm, rh]
    return lax.dot_general(
        jnp.concatenate(lefts, axis=0), jnp.concatenate(rights, axis=0), (((0,), (0,)), ((), ())),
        preferred_element_type=F32,
    )


def sweep_inverse(blocks):
    groups = PANEL // 8
    sub = lax.broadcasted_iota(jnp.int32, (8, HALF), 0)
    lane = lax.broadcasted_iota(jnp.int32, (8, HALF), 1)
    all_lanes = lax.broadcasted_iota(jnp.int32, (HALF, HALF), 1)

    def splat(value, row):
        return jnp.broadcast_to(value[row : row + 1, :], (8, HALF))

    def columns_of(rows, at):
        return tuple(
            tuple(jnp.broadcast_to(rows[8 * g : 8 * g + 8, at + j : at + j + 1], (8, HALF)) for g in range(groups))
            for j in range(PANEL)
        )

    def pivots(a, cols):
        cols = [list(c) for c in cols]
        top = [jnp.where(lane < PANEL, (lane == sub + 8 * g).astype(F32), a[8 * g : 8 * g + 8, :]) for g in range(groups)]
        for k in range(PANEL):
            at, row = k // 8, k % 8
            here = cols[k]
            inv = 1.0 / splat(here[at], row)
            hit = sub == row
            scaled = [jnp.where(hit, -inv, here[g] * inv) if g == at else here[g] * inv for g in range(groups)]

            def eliminate(target):
                lead = splat(target[at], row)
                return [
                    (jnp.where(hit, 0.0, target[g]) if g == at else target[g]) - scaled[g] * lead for g in range(groups)
                ]

            for j in range(k + 1, PANEL):
                cols[j] = eliminate(cols[j])
            top = eliminate(top)
        return jnp.concatenate([jnp.where(lane < PANEL, -t, t) for t in top], axis=0)

    def update(a, top, near):
        ahead = [jnp.where(lane < PANEL, 0.0, a[PANEL + 8 * g : PANEL + 8 * g + 8, :]) for g in range(groups)]
        for g in range(groups):
            terms = [near[k][g] * splat(top[8 * (k // 8) : 8 * (k // 8) + 8, :], k % 8) for k in range(PANEL)]
            while len(terms) > 1:
                terms = [terms[i] + terms[i + 1] for i in range(0, len(terms), 2)]
            ahead[g] = ahead[g] - terms[0]
        ahead = jnp.concatenate(ahead, axis=0)
        below = jnp.where(all_lanes[2 * PANEL :, :] < PANEL, 0.0, a[2 * PANEL :, :]) - wide_dot([a[0:PANEL, 2 * PANEL :]], [top])
        cols = columns_of(ahead, PANEL)
        return pltpu.roll(jnp.concatenate([ahead, below, top], axis=0), HALF - PANEL, 1), cols

    def panel(_, state):
        out = []
        for a, cols in state:
            near = columns_of(a[PANEL : 2 * PANEL, :], 0)
            top = pivots(a, cols)
            out.append(update(a, top, near))
        return tuple(out)

    start = tuple((a, columns_of(a[0:PANEL, :], 0)) for a in blocks)
    return [-a for a, _ in lax.fori_loop(0, HALF // PANEL, panel, start, unroll=UNROLL)]


def sweep_pair(first, second, store):
    groups = PANEL // 8
    side = HALF // 2
    per_side = side // PANEL
    steps = HALF // PANEL
    sub = lax.broadcasted_iota(jnp.int32, (8, HALF), 0)
    lane = lax.broadcasted_iota(jnp.int32, (8, HALF), 1)
    shift = jnp.where(lane < side, 0, side)
    at_lane = lane - shift
    left_rows = lax.broadcasted_iota(jnp.int32, (PANEL, HALF), 1) < side
    wide_lane = lax.broadcasted_iota(jnp.int32, (HALF, HALF), 1)
    left_wide = wide_lane < side
    wide_at = jnp.where(left_wide, wide_lane, wide_lane - side)

    def splat(value, row):
        return jnp.broadcast_to(value[row : row + 1, :], (8, HALF))

    def columns_at(rows, p):
        source = jnp.where(p % (2 * per_side) < per_side, rows[0], rows[1])
        base = lax.rem(p, per_side) * PANEL
        return tuple(
            tuple(
                jnp.take_along_axis(source[8 * g : 8 * g + 8, :], shift + (base + j), axis=1, mode="promise_in_bounds")
                for g in range(groups)
            )
            for j in range(PANEL)
        )

    def inside(lanes, v, p):
        start = p * PANEL - v * side
        return (lanes >= start) & (lanes < start + PANEL)

    def pivots(rows, cols, p):
        cols = [list(c) for c in cols]
        tops = []
        for v in range(2):
            start = p * PANEL - v * side
            tops.append([
                jnp.where(inside(at_lane, v, p), (at_lane == sub + (start + 8 * g)).astype(F32), rows[v][8 * g : 8 * g + 8, :])
                for g in range(groups)
            ])
        for k in range(PANEL):
            at, row = k // 8, k % 8
            here = cols[k]
            inv = 1.0 / splat(here[at], row)
            hit = sub == row
            scaled = [jnp.where(hit, -inv, here[g] * inv) if g == at else here[g] * inv for g in range(groups)]

            def eliminate(target):
                lead = splat(target[at], row)
                return [
                    (jnp.where(hit, 0.0, target[g]) if g == at else target[g]) - scaled[g] * lead for g in range(groups)
                ]

            for j in range(k + 1, PANEL):
                cols[j] = eliminate(cols[j])
            tops = [eliminate(top) for top in tops]
        return [
            jnp.concatenate([jnp.where(inside(at_lane, v, p), -t, t) for t in tops[v]], axis=0) for v in range(2)
        ]

    def panel(p, state):
        rows, cols = state
        following = pl.ds(pl.multiple_of(jnp.minimum(p + 1, steps - 1) * PANEL, PANEL), PANEL)
        after = [store[v, following, :] for v in range(2)]
        near = columns_at(after, p)
        tops = pivots(rows, cols, p)
        ahead = []
        for v in range(2):
            parts = []
            for g in range(groups):
                terms = [near[k][g] * splat(tops[v][8 * (k // 8) : 8 * (k // 8) + 8, :], k % 8) for k in range(PANEL)]
                while len(terms) > 1:
                    terms = [terms[i] + terms[i + 1] for i in range(0, len(terms), 2)]
                parts.append(jnp.where(inside(at_lane, v, p), 0.0, after[v][8 * g : 8 * g + 8, :]) - terms[0])
            ahead.append(jnp.concatenate(parts, axis=0))
        one = jnp.where(left_rows, rows[0], pltpu.roll(rows[1], side, 1))
        two = jnp.where(left_rows, pltpu.roll(rows[0], side, 1), rows[1])
        for v in range(2):
            change = wide_dot([one, two], [jnp.where(left_rows, tops[v], 0.0), jnp.where(left_rows, 0.0, tops[v])])
            store[v] = jnp.where(inside(wide_at, v, p), 0.0, store[v]) - change
            store[v, pl.ds(pl.multiple_of(p * PANEL, PANEL), PANEL), :] = tops[v]
        return ahead, columns_at(ahead, p + 1)

    store[0] = jnp.where(left_wide, first, pltpu.roll(second, side, 1))
    store[1] = jnp.where(left_wide, pltpu.roll(first, side, 1), second)
    rows = [store[v, 0:PANEL, :] for v in range(2)]
    lax.fori_loop(0, steps, panel, (rows, columns_at(rows, 0)), unroll=UNROLL)
    return [
        -jnp.where(left_wide, store[0], pltpu.roll(store[1], side, 1)),
        -jnp.where(left_wide, pltpu.roll(store[0], side, 1), store[1]),
    ]


def high_dot(a, b, contract):
    return lax.dot_general(a, b, (contract, ((), ())), precision=HIGHEST, preferred_element_type=F32)


def invert_dense(m11, m21, m22, store):
    count = len(m11)

    def sweep(blocks):
        return sweep_pair(*blocks, store) if count == 2 else sweep_inverse(blocks)

    x11 = sweep(m11)
    g = [high_dot(m21[i], x11[i], ((1,), (0,))) for i in range(count)]
    y = sweep([m22[i] - high_dot(g[i], m21[i], ((1,), (1,))) for i in range(count)])
    b21 = [-high_dot(y[i], g[i], ((1,), (0,))) for i in range(count)]
    b11 = [x11[i] - high_dot(g[i], b21[i], ((0,), (0,))) for i in range(count)]
    return b11, b21, y


def invert_parts(values, tokens, store):
    rows, cols = square_iota()
    eye = rows == cols
    m11, m21, m22 = [], [], []
    for value in values:
        p11, p21, p22 = unpack(value / tokens)
        damping = damping_ratio * jnp.sum(jnp.where(eye, p11 + p22, 0.0), axis=(0, 1), keepdims=True) / BLK
        m11.append(p11 + jnp.where(eye, damping, 0.0))
        m21.append(p21)
        m22.append(p22 + jnp.where(eye, damping, 0.0))
    return invert_dense(m11, m21, m22, store)


def solve_kernel(n, sections, nblocks, tokens, acts, grad, precond, rows_out, acts_v, grad_v, theirs, mine, from_pair,
                 inbound, landed, full, store, acts_s, grad_s, pair_s, pair_r, sum_s, sum_r, line_s, swap_s, near_r,
                 side_s, side_r):
    chips = n // 2
    nhalf = nblocks // 2
    nown = -(-nhalf // 2)
    share = BLK // n
    me = lax.axis_index("dp")
    section = lax.axis_index("pipe")
    core = lax.rem(me, 2)
    chip = me // 2
    pair = me + 1 - 2 * core
    low = (jnp.maximum(chip - 1, 0)) * 2 + core
    high = (jnp.minimum(chip + 1, chips - 1)) * 2 + core
    first = chip == 0
    last = chip == chips - 1
    is_last = last.astype(jnp.int32)

    def acts_copy(t):
        span = pl.ds(pl.multiple_of(t * 2 * BLK, 2 * BLK), 2 * BLK)
        return pltpu.make_async_copy(acts.at[:, span], acts_v.at[:, span], acts_s.at[t])

    def turn_of(p):
        natural = p
        up_first = jnp.where(p < nhalf // 2, 2 * p + 1, 2 * (p - nhalf // 2))
        down_first = jnp.where(p < nown, 2 * p, 2 * (p - nown) + 1)
        return jnp.where(first, up_first, jnp.where(last, down_first, natural))

    greet_wait = greet(
        [(None, {"dp": pair}), (chip > 0, {"dp": low}), (chip < chips - 1, {"dp": high})]
        + [(None, {"pipe": lax.rem(section + step, sections)}) for step in range(1, sections)]
    )

    for p in range(nhalf):
        acts_copy(turn_of(p)).start()
    grad_copy = pltpu.make_async_copy(grad, grad_v, grad_s)
    grad_copy.start()

    def partial(block, ref):
        x = acts_v[:, pl.ds(pl.multiple_of(block * BLK, BLK), BLK)]
        whole = lax.dot_general(x, x, (((0,), (0,)), ((), ())), preferred_element_type=F32)
        pack_into(ref, whole[0:HALF, 0:HALF], whole[HALF:BLK, 0:HALF], whole[HALF:BLK, HALF:BLK])

    def pair_copy(t):
        return pltpu.make_async_remote_copy(
            src_ref=theirs.at[t], dst_ref=from_pair.at[t], send_sem=pair_s.at[t], recv_sem=pair_r.at[t],
            device_id={"dp": pair}, device_id_type=MESH,
        )

    def fold_pair(t):
        pair_copy(t).wait()
        mine[t] = mine[t] + from_pair[t]

    def piece(k):
        return pl.ds(*PIECES[k])

    def sum_copy(t, k, target):
        return pltpu.make_async_remote_copy(
            src_ref=mine.at[t, piece(k)], dst_ref=inbound.at[t, piece(k)], send_sem=sum_s.at[t, k],
            recv_sem=sum_r.at[t, k], device_id={"dp": target}, device_id_type=MESH,
        )

    def pass_sum(t, k, heads, target):
        @pl.when(jnp.logical_not(heads))
        def _():
            sum_copy(t, k, target).wait_recv()
            mine[t, piece(k)] = mine[t, piece(k)] + inbound[t, piece(k)]

        sum_copy(t, k, target).start()

    def take_turn(p):
        t = turn_of(p)
        acts_copy(t).wait()
        partial(2 * t + 1 - core, theirs.at[t])
        pair_copy(t).start()
        partial(2 * t + core, mine.at[t])

    start_t = turn_of(0)
    acts_copy(start_t).wait()
    partial(2 * start_t + 1 - core, theirs.at[start_t])
    partial(2 * start_t + core, mine.at[start_t])
    greet_wait()
    pair_copy(start_t).start()

    @pl.loop(0, nown + chips)
    def _(tick):
        @pl.when(2 * tick + 1 < nhalf)
        def _():
            take_turn(2 * tick + 1)

        i = tick - chip
        t = 2 * i + 1
        rising = (i >= 0) & (t < nhalf) & jnp.logical_not(last)
        j = tick - (chips - 1 - chip)
        u = 2 * j
        falling = (j >= 0) & (u < nhalf) & jnp.logical_not(first)

        @pl.when(rising)
        def _():
            fold_pair(t)

        @pl.when(falling)
        def _():
            fold_pair(u)

        for k in range(CHUNKS):
            @pl.when(rising)
            def _():
                pass_sum(t, k, first, high)

            @pl.when(falling)
            def _():
                pass_sum(u, k, last, low)

        @pl.when(2 * tick + 2 < nhalf)
        def _():
            take_turn(2 * tick + 2)

    def close_sum(t):
        fold_pair(t)
        for k in range(CHUNKS):
            sum_copy(t, k, low).wait_recv()
        return mine[t] + inbound[t]

    def invert(slots):
        own = [2 * slot + is_last for slot in slots]
        b11, b21, b22 = invert_parts([close_sum(t) for t in own], tokens, store)
        for i, t in enumerate(own):
            pack_into(landed.at[2 * t + core], b11[i], b21[i], b22[i])

    def send(t, half, k, target, sem):
        block = 2 * t + half
        return pltpu.make_async_remote_copy(
            src_ref=landed.at[block, piece(k)], dst_ref=landed.at[block, piece(k)], send_sem=sem.at[t, k],
            recv_sem=near_r.at[block, k], device_id={"dp": target}, device_id_type=MESH,
        )

    def flow(t, k, owned, ends, target):
        @pl.when(jnp.logical_not(owned))
        def _():
            send(t, core, k, pair, swap_s).wait_recv()

        @pl.when(jnp.logical_not(ends))
        def _():
            send(t, core, k, target, line_s).start()

        send(t, core, k, pair, swap_s).start()

    def side(block, step):
        mine_rows = full.at[block, pl.ds(pl.multiple_of(me * share, share), share), :]
        return pltpu.make_async_remote_copy(
            src_ref=mine_rows, dst_ref=rows_out.at[section, block], send_sem=side_s.at[block, step - 1],
            recv_sem=side_r.at[section, block],
            device_id={"pipe": lax.rem(section + step, sections)}, device_id_type=MESH,
        )

    def open_block(block):
        m11, m21, m22 = unpack(landed[block])
        full[block, 0:HALF, 0:HALF] = m11
        full[block, HALF:BLK, 0:HALF] = m21
        full[block, 0:HALF, HALF:BLK] = m21.T
        full[block, HALF:BLK, HALF:BLK] = m22
        for step in range(1, sections):
            side(block, step).start()
        rows_out[section, block] = full[block, pl.ds(pl.multiple_of(me * share, share), share), :]

    def open_other(t):
        for k in range(CHUNKS):
            send(t, 1 - core, k, pair, swap_s).wait_recv()
        open_block(2 * t + 1 - core)

    def product(block):
        span = pl.ds(pl.multiple_of(block * BLK, BLK), BLK)
        a = full[block]
        b = grad_v[span, :]
        a_high = a.astype(BF16)
        a_low = (a - a_high.astype(F32)).astype(BF16)
        b_high = b.astype(BF16)
        b_low = (b - b_high.astype(F32)).astype(BF16)
        small = jnp.dot(a_high, b_low, preferred_element_type=F32) + jnp.dot(a_low, b_high, preferred_element_type=F32)
        precond[span, :] = jnp.dot(a_high, b_high, preferred_element_type=F32) + small

    def both_products(t):
        @pl.loop(0, 2)
        def _(half):
            product(2 * t + half)

    @pl.loop(0, nown + chips)
    def _(tick):
        i = tick - chip
        t = 2 * i
        rising = (i >= 0) & (t < nhalf)
        j = tick - (chips - 1 - chip)
        u = 2 * j + 1
        falling = (j >= 0) & (u < nhalf)
        rose = (i >= 1) & (t - 2 < nhalf)
        fell = (j >= 1) & (u - 2 < nhalf)

        @pl.when((tick == 0) & (first | last))
        def _():
            invert([0])

        @pl.when((tick == 1) & (first | last))
        def _():
            invert(list(range(1, nown)))

        for k in range(CHUNKS):
            @pl.when(rising)
            def _():
                flow(t, k, first, last, high)

            @pl.when(falling)
            def _():
                flow(u, k, last, first, low)

            if k == 0:
                @pl.when(rose)
                def _():
                    open_other(t - 2)

                @pl.when(fell)
                def _():
                    open_other(u - 2)

                @pl.when(tick == 1)
                def _():
                    grad_copy.wait()

            if k == CHUNKS // 2:
                @pl.when(rose)
                def _():
                    both_products(t - 2)

            if k == CHUNKS - 1:
                @pl.when(rising)
                def _():
                    open_block(2 * t + core)

                @pl.when(falling)
                def _():
                    open_block(2 * u + core)

                @pl.when(fell)
                def _():
                    both_products(u - 2)

    @pl.loop(0, nhalf)
    def _(t):
        odd = lax.rem(t, 2) == 1
        sends_sum = jnp.where(odd, jnp.logical_not(last), jnp.logical_not(first))
        sends_inverse = jnp.where(odd, jnp.logical_not(first), jnp.logical_not(last))
        for k in range(CHUNKS):
            @pl.when(sends_sum)
            def _():
                sum_copy(t, k, low).wait_send()

            @pl.when(sends_inverse)
            def _():
                send(t, core, k, low, line_s).wait_send()

            send(t, core, k, pair, swap_s).wait_send()

    @pl.loop(0, nblocks)
    def _(block):
        for step in range(1, sections):
            side(block, step).wait_send()
            source = lax.rem(section + step, sections)
            pltpu.make_async_remote_copy(
                src_ref=rows_out.at[source, block], dst_ref=rows_out.at[source, block],
                send_sem=side_s.at[block, step - 1], recv_sem=side_r.at[source, block],
                device_id={"pipe": source}, device_id_type=MESH,
            ).wait_recv()


def emit_kernel(owner_of, values, rows, precond, held, owners, slots, zeros, copy_s, held_s, owner_s):
    section = lax.axis_index("pipe")
    sections, nblocks = owner_of.shape
    total = sections * nblocks
    owner_copy = pltpu.make_async_copy(owner_of, owners, owner_s)
    owner_copy.start()
    zeros[...] = jnp.zeros_like(zeros)

    def precond_copy(b):
        span = pl.ds(pl.multiple_of(b * BLK, BLK), BLK)
        return pltpu.make_async_copy(values.at[span, :], precond.at[span, :], copy_s.at[b])

    for b in range(nblocks):
        precond_copy(b).start()

    for j in range(HOST):
        slots[j] = -1
    owner_copy.wait()

    def place(k, used):
        hit = owners[k // nblocks, lax.rem(k, nblocks)] == section

        @pl.when(hit)
        def _():
            slots[used] = k

        return used + hit.astype(jnp.int32)

    lax.fori_loop(0, total, place, jnp.int32(0))

    @pl.loop(0, HOST)
    def _(j):
        k = slots[j]

        @pl.when(k >= 0)
        def _():
            pltpu.make_async_copy(rows.at[k // nblocks, lax.rem(k, nblocks)], held.at[j], held_s.at[j]).start()

        @pl.when(k < 0)
        def _():
            pltpu.make_async_copy(zeros, held.at[j], held_s.at[j]).start()

    @pl.loop(0, HOST)
    def _(j):
        pltpu.make_async_copy(zeros, held.at[j], held_s.at[j]).wait()

    for b in range(nblocks):
        precond_copy(b).wait()


def shards(acts, grad, owner_of):
    tokens, feature_count = acts.shape[1:]
    columns = grad.shape[1]
    nblocks = feature_count // BLK
    n = lax.axis_size("dp")
    sections = lax.axis_size("pipe")
    nhalf = nblocks // 2
    share = BLK // n
    vmem = pl.BlockSpec(memory_space=pltpu.VMEM)
    hbm = pl.BlockSpec(memory_space=pltpu.HBM)
    dma = pltpu.SemaphoreType.DMA

    values, rows = pl.pallas_call(
        functools.partial(solve_kernel, n, sections, nblocks, float(tokens * n)),
        out_shape=(
            pltpu.VMEM((feature_count, columns), F32),
            pltpu.VMEM((sections, nblocks, share, BLK), F32),
        ),
        in_specs=[hbm, hbm],
        out_specs=(vmem, vmem),
        scratch_shapes=[
            pltpu.VMEM((tokens, feature_count), BF16),
            pltpu.VMEM((feature_count, columns), F32),
            pltpu.VMEM((nhalf, PACK, HALF), F32),
            pltpu.VMEM((nhalf, PACK, HALF), F32),
            pltpu.VMEM((nhalf, PACK, HALF), F32),
            pltpu.VMEM((nhalf, PACK, HALF), F32),
            pltpu.VMEM((nblocks, PACK, HALF), F32),
            pltpu.VMEM((nblocks, BLK, BLK), F32),
            pltpu.VMEM((2, HALF, HALF), F32),
            dma((nhalf,)), dma, dma((nhalf,)), dma((nhalf,)), dma((nhalf, CHUNKS)), dma((nhalf, CHUNKS)),
            dma((nhalf, CHUNKS)), dma((nhalf, CHUNKS)), dma((nblocks, CHUNKS)),
            dma((nblocks, sections - 1)), dma((sections, nblocks)),
        ],
        compiler_params=pltpu.CompilerParams(collective_id=0, has_side_effects=True, vmem_limit_bytes=36 * 2**20),
        name="solve_blocks",
    )(pltpu.with_memory_space_constraint(acts[0], pltpu.HBM), pltpu.with_memory_space_constraint(grad, pltpu.HBM))

    precond, held = pl.pallas_call(
        emit_kernel,
        in_specs=[hbm, vmem, vmem],
        out_specs=(hbm, hbm),
        out_shape=(
            jax.ShapeDtypeStruct((feature_count, columns), F32),
            jax.ShapeDtypeStruct((HOST, share, BLK), F32),
        ),
        scratch_shapes=[
            pltpu.SMEM(owner_of.shape, jnp.int32), pltpu.SMEM((HOST,), jnp.int32), pltpu.VMEM((share, BLK), F32),
            dma((nblocks,)), dma((HOST,)), dma,
        ],
        compiler_params=pltpu.CompilerParams(vmem_limit_bytes=16 * 2**20),
        name="emit_outputs",
    )(pltpu.with_memory_space_constraint(owner_of, pltpu.HBM), values, rows)
    return precond, held[None]


def solution(mesh):
    placed = (P("pipe", "dp", None), P("pipe", "dp"), P())
    return jax.shard_map(
        shards,
        mesh=mesh,
        in_specs=placed,
        out_specs=(P("pipe", "dp"), P("pipe", None, "dp", None)),
        check_vma=False,
    )
```
